32 devices in a mesh: fsdp: 4 (over y, x), tp: 8 (over z, core).
Axes of the slice: x: 2, y: 2, z: 4, core: 2. Of those that a mesh axis runs over, the one named last changes fastest.
Arguments:
- tokens: bfloat16 [1024, 8192], P('fsdp', 'tp'), may hold values from -6 to 6
- out_grad: bfloat16 [1024, 8192], P('fsdp', 'tp'), may hold values from -6 to 6
- gate_weight: bfloat16 [8192, 1024], P('fsdp', 'tp'), may hold values from -0.0625 to 0.0625
- up_weight: bfloat16 [8192, 1024], P('fsdp', 'tp'), may hold values from -0.0625 to 0.0625
- down_weight: bfloat16 [1024, 8192], P('tp', 'fsdp'), may hold values from -0.1875 to 0.1875
Outputs:
- input_grad: bfloat16 [1024, 8192], P('fsdp', 'tp')
- gate_grad: float32 [8192, 1024], P('fsdp', 'tp')
- up_grad: float32 [8192, 1024], P('fsdp', 'tp')
- down_grad: float32 [1024, 8192], P('tp', 'fsdp')
The draws below stay inside these ranges and needn't reach their ends.
All inputs are finite; a program needn't handle non-finite values.
Results may differ from the reference program's by a relative error of at most 0.0023.
Values may be sent and summed in bfloat16 or wider, within the bound.
A program may use at most 128 MiB of HBM per device.

```python
import math
import jax
import jax.numpy as jnp

D = 8192
FF_WIN = 1024
TOKENS = 1024


def spiked(values, stream_key, source, target, blocks, factor):
    def block_of(dim):
        return (jnp.arange(values.shape[dim]) // (values.shape[dim] // blocks)).reshape((-1,) + (1,) * (values.ndim - 1 - dim))

    one_side = jax.random.permutation(stream_key, blocks)[block_of(target)]
    other_side = (block_of(target) + blocks // 2) % blocks
    return jnp.where((block_of(source) == one_side) | (block_of(source) == other_side), factor * values, values)


def level_of(key, dims, shards, low, largest):
    factor_of = 1.0
    for dim, shards_of in shards:
        heights = jax.random.uniform(jax.random.fold_in(jax.random.fold_in(key, 6), dim), (shards_of,), jnp.float32, low / len(shards), largest / len(shards))
        factor_of = factor_of * jnp.repeat(jnp.exp(heights), dims[dim] // shards_of).reshape((-1,) + (1,) * (len(dims) - 1 - dim))
    return factor_of


def gaussian(key, extent, deviation, bound, pieces=(), dtype=jnp.bfloat16):
    array = jax.random.normal(key, extent, jnp.float32) * deviation
    if len(pieces) > 0:
        array = level_of(key, extent, pieces, -0.22, 0.18) * array
    return jnp.clip(array, min=-bound, max=bound).astype(dtype)


def bell_draw_with(rng, shape, width, most, split, heavy, kind=jnp.bfloat16):
    result = width * jax.random.normal(rng, shape, jnp.float32)
    if split:
        result = result * level_of(rng, shape, split, -0.22, 0.18)
    return jnp.clip(spiked(result, jax.random.fold_in(rng, 3), *heavy), -most, most).astype(kind)


def setup_inputs(seed: int = 0) -> dict:
    seeds = jax.random.split(jax.random.key(seed), 6)
    return {
        "tokens": bell_draw_with(seeds[0], (TOKENS, D), 1.0, 6.0, ((0, 4), (1, 8)), (0, 1, 8, 2.0)),
        "out_grad": bell_draw_with(seeds[1], (TOKENS, D), 1.0, 6.0, ((0, 4), (1, 8)), (0, 1, 8, 2.0)),
        "gate_weight": gaussian(seeds[2], (D, FF_WIN), D ** -0.5, 0.0625, ((0, 4), (1, 8))),
        "up_weight": gaussian(seeds[3], (D, FF_WIN), D ** -0.5, 0.0625, ((0, 4), (1, 8))),
        "down_weight": gaussian(seeds[4], (FF_WIN, D), FF_WIN ** -0.5, 0.1875, ((0, 8), (1, 4))),
    }


def reference(tokens, out_grad, gate_weight, up_weight, down_weight):
    gate = jnp.dot(tokens, gate_weight, preferred_element_type=jnp.float32)
    up = jnp.dot(tokens, up_weight, preferred_element_type=jnp.float32)
    squashed = jax.nn.sigmoid(gate)
    activated = gate * squashed
    slope = squashed * (1.0 + gate * (1.0 - squashed))
    hidden = (activated * up).astype(jnp.bfloat16)
    hidden_grad = jnp.dot(out_grad, down_weight.T, preferred_element_type=jnp.float32)
    gate_delta = (hidden_grad * up * slope).astype(jnp.bfloat16)
    up_delta = (hidden_grad * activated).astype(jnp.bfloat16)
    input_grad = jnp.dot(gate_delta, gate_weight.T, preferred_element_type=jnp.float32)
    input_grad = input_grad + jnp.dot(up_delta, up_weight.T, preferred_element_type=jnp.float32)
    factor = 1.0 / math.sqrt(TOKENS)
    gate_grad = jnp.dot(tokens.T, gate_delta, preferred_element_type=jnp.float32) * factor
    up_grad = jnp.dot(tokens.T, up_delta, preferred_element_type=jnp.float32) * factor
    down_grad = jnp.dot(hidden.T, out_grad, preferred_element_type=jnp.float32) * factor
    return (input_grad.astype(jnp.bfloat16), gate_grad, up_grad, down_grad)
```

```python
import functools
import math

import jax
import jax.numpy as jnp
from jax import lax
from jax.sharding import PartitionSpec as P
from jax.experimental import pallas as pl
from jax.experimental.pallas import tpu as pltpu

MESH = pl.DeviceIdType.MESH
F32 = jnp.float32
BF16 = jnp.bfloat16
VMEM_LIMIT = 60 * 1024 * 1024


def place(nf, nt):
    return lax.axis_index("fsdp"), lax.axis_index("tp")


def enter(nf, nt):
    f, t = place(nf, nt)
    barrier = pltpu.get_barrier_semaphore()
    for j in range(1, nf):
        pl.semaphore_signal(
            barrier, inc=1, device_id=(lax.rem(f + j, nf), t), device_id_type=MESH
        )
    for j in range(1, nt):
        pl.semaphore_signal(
            barrier, inc=1, device_id=(f, lax.rem(t + j, nt)), device_id_type=MESH
        )
    pl.semaphore_wait(barrier, nf + nt - 2)


def remote(src, dst, send, recv, device):
    return pltpu.make_async_remote_copy(
        src_ref=src,
        dst_ref=dst,
        send_sem=send,
        recv_sem=recv,
        device_id=device,
        device_id_type=MESH,
    )


def line_steps(stage, mats, nz, f, t, up_send, down_send, recv, arrived):
    z = t // 2

    def up(m, b):
        return remote(
            stage.at[m, b], stage.at[m, b], up_send.at[m, b], recv.at[m, b], (f, t + 2)
        )

    def down(m, b):
        return remote(
            stage.at[m, b], stage.at[m, b], down_send.at[m, b], recv.at[m, b], (f, t - 2)
        )

    for s in range(nz):
        for m in range(mats):
            for direction in (0, 1) if s else (0,):
                b = z - s if direction == 0 else z + s

                @pl.when((b >= 0) & (b < nz))
                def _(m=m, b=b, s=s, direction=direction):
                    if s:
                        up(m, b).wait_recv()
                    if s == 0 or direction == 0:

                        @pl.when(z < nz - 1)
                        def _():
                            up(m, b).start()

                    if s == 0 or direction == 1:

                        @pl.when(z > 0)
                        def _():
                            down(m, b).start()

                    arrived(m, b)

    def finish():
        for b in range(nz):
            for m in range(mats):

                @pl.when((z < nz - 1) & (b <= z))
                def _(m=m, b=b):
                    up(m, b).wait_send()

                @pl.when((z > 0) & (b >= z))
                def _(m=m, b=b):
                    down(m, b).wait_send()

    return finish


def spread_kernel(
    nf,
    nt,
    tokens,
    grads,
    weights,
    x_out,
    g_out,
    w_out,
    stage,
    local_sem,
    up_send,
    down_send,
    line_recv,
    plane_send,
    plane_recv,
    pair_send,
    pair_recv,
    w_send,
    w_recv,
):
    f, t = place(nf, nt)
    nz = nt // 2
    z, k = t // 2, lax.rem(t, 2)
    rows, width = tokens.shape
    outs = (x_out, g_out)
    loads = []
    for m, ref in enumerate((tokens, grads)):
        load = pltpu.make_async_copy(ref, stage.at[m, z], local_sem.at[m])
        load.start()
        loads.append(load)
    part = w_out.shape[0]
    depth = weights.shape[1]
    w_own = pltpu.make_async_copy(
        weights.at[pl.ds(t * part, part)],
        w_out.at[:, pl.ds(pl.multiple_of(t * depth, depth), depth)],
        local_sem.at[2],
    )
    w_own.start()
    enter(nf, nt)
    for load in loads:
        load.wait()

    half = pl.ds(pl.multiple_of(k * width, width), width)

    def spot(m, g):
        return outs[m].at[pl.ds(pl.multiple_of(g * rows, rows), rows), half]

    def plane(m, b):
        return remote(
            stage.at[m, b], spot(m, f), plane_send.at[m, b], plane_recv.at[m, f], (b, t)
        )

    def plane_in(m, g):
        return remote(
            stage.at[m, 0], spot(m, g), plane_send.at[m, 0], plane_recv.at[m, g], (f, t)
        )

    def keep(m):
        return pltpu.make_async_copy(stage.at[m, f], spot(m, f), plane_recv.at[m, f])

    def arrived(m, b):
        @pl.when(b != f)
        def _():
            plane(m, b).start()

        @pl.when(b == f)
        def _():
            keep(m).start()

    finish = line_steps(
        stage, 2, nz, f, t, up_send, down_send, line_recv, arrived
    )

    def w_copy(u):
        return remote(
            weights.at[pl.ds(u * part, part)],
            w_out.at[:, pl.ds(pl.multiple_of(t * depth, depth), depth)],
            w_send.at[u],
            w_recv.at[t],
            (f, u),
        )

    def w_in(u):
        return remote(
            weights.at[pl.ds(0, part)],
            w_out.at[:, pl.ds(pl.multiple_of(u * depth, depth), depth)],
            w_send.at[u],
            w_recv.at[u],
            (f, u),
        )

    for j in range(1, nt):
        w_copy(lax.rem(t + j, nt)).start()

    def pair(m, g):
        return remote(
            spot(m, g), spot(m, g), pair_send.at[m, g], pair_recv.at[m, g], (f, t + 1 - 2 * k)
        )

    for m in range(2):
        for j in range(nf):
            g = lax.rem(f + j, nf)
            if j == 0:
                keep(m).wait()
            else:
                plane_in(m, g).wait_recv()
            pair(m, g).start()
    finish()
    for m in range(2):
        for b in range(nz):

            @pl.when(b != f)
            def _(m=m, b=b):
                plane(m, b).wait_send()

        for g in range(nf):
            pair(m, g).wait()
    w_own.wait()
    for j in range(1, nt):
        u = lax.rem(t + j, nt)
        w_copy(u).wait_send()
        w_in(u).wait_recv()


def middle_kernel(
    nf,
    nt,
    partial,
    all_out,
    hidden_out,
    landing,
    stage,
    hidden_own,
    sum_send,
    sum_recv,
    up_send,
    down_send,
    line_recv,
    plane_send,
    plane_recv,
    pair_send,
    pair_recv,
    h_send,
    h_recv,
    local_sem,
):
    f, t = place(nf, nt)
    nz = nt // 2
    z, k = t // 2, lax.rem(t, 2)
    rows = landing.shape[1]
    width = hidden_own.shape[1]

    def block(g):
        return pl.ds(pl.multiple_of(g * rows, rows), rows)

    enter(nf, nt)

    def share(g):
        return remote(
            partial.at[block(g)], landing.at[f], sum_send.at[g], sum_recv.at[f], (g, t)
        )

    def share_in(g):
        return remote(
            partial.at[block(g)], landing.at[g], sum_send.at[g], sum_recv.at[g], (g, t)
        )

    for j in range(1, nf):
        share(lax.rem(f + j, nf)).start()
    for j in range(1, nf):
        share_in(lax.rem(f + j, nf)).wait_recv()
    total = partial[block(f), :]
    for j in range(1, nf):
        total = total + landing[lax.rem(f + j, nf)]
    gate = total[:, :width]
    up = total[:, width : 2 * width]
    hidden_grad = total[:, 2 * width :]
    squashed = jax.nn.sigmoid(gate)
    activated = gate * squashed
    slope = squashed * (1.0 + gate * (1.0 - squashed))
    stage[0, z, :, :width] = (hidden_grad * up * slope).astype(BF16)
    stage[0, z, :, width:] = (hidden_grad * activated).astype(BF16)
    hidden_own[...] = (activated * up).astype(BF16)

    def h_copy(g):
        return remote(
            hidden_own, hidden_out.at[block(f)], h_send.at[g], h_recv.at[f], (g, t)
        )

    def h_in(g):
        return remote(
            hidden_own, hidden_out.at[block(g)], h_send.at[g], h_recv.at[g], (g, t)
        )

    def spot(g, b):
        at = pl.multiple_of((2 * b + k) * 2 * width, 2 * width)
        return all_out.at[block(g), pl.ds(at, 2 * width)]

    def plane(b, g):
        return remote(
            stage.at[0, b], spot(f, b), plane_send.at[b, g], plane_recv.at[b, f], (g, t)
        )

    def plane_in(b, g):
        return remote(
            stage.at[0, b], spot(g, b), plane_send.at[b, g], plane_recv.at[b, g], (g, t)
        )

    def keep(b):
        return pltpu.make_async_copy(stage.at[0, b], spot(f, b), plane_recv.at[b, f])

    def arrived(m, b):
        for j in range(1, nf):
            plane(b, lax.rem(f + j, nf)).start()
        keep(b).start()

    finish = line_steps(stage, 1, nz, f, t, up_send, down_send, line_recv, arrived)
    for j in range(1, nf):
        h_copy(lax.rem(f + j, nf)).start()
    h_keep = pltpu.make_async_copy(hidden_own, hidden_out.at[block(f)], local_sem.at[0])
    h_keep.start()

    def pair(b, g):
        return remote(
            spot(g, b), spot(g, b), pair_send.at[b, g], pair_recv.at[b, g], (f, t + 1 - 2 * k)
        )

    def pair_in(b, g):
        at = pl.multiple_of((2 * b + 1 - k) * 2 * width, 2 * width)
        here = all_out.at[block(g), pl.ds(at, 2 * width)]
        return remote(
            here, here, pair_send.at[b, g], pair_recv.at[b, g], (f, t + 1 - 2 * k)
        )

    for b in range(nz):
        for j in range(nf):
            g = lax.rem(f + j, nf)
            if j == 0:
                keep(b).wait()
            else:
                plane_in(b, g).wait_recv()
            pair(b, g).start()
    finish()
    h_keep.wait()
    for j in range(1, nf):
        g = lax.rem(f + j, nf)
        share(g).wait_send()
        h_copy(g).wait_send()
        h_in(g).wait_recv()
        for b in range(nz):
            plane(b, g).wait_send()
    for b in range(nz):
        for g in range(nf):
            pair(b, g).wait_send()
            pair_in(b, g).wait_recv()


def return_kernel(nf, nt, result, out, landing, send, recv, send2, recv2, local_sem):
    f, t = place(nf, nt)
    rows = landing.shape[1]

    def block(g):
        return pl.ds(pl.multiple_of(g * rows, rows), rows)

    keep = pltpu.make_async_copy(result.at[block(f)], landing.at[f], local_sem.at[0])
    keep.start()
    enter(nf, nt)

    def first(g):
        return remote(result.at[block(g)], landing.at[f], send.at[g], recv.at[f], (g, t))

    def first_in(g):
        return remote(result.at[block(g)], landing.at[g], send.at[g], recv.at[g], (g, t))

    for j in range(1, nf):
        first(lax.rem(f + j, nf)).start()
    keep.wait()
    lane = lax.rem(t, nf)

    def second(g):
        return remote(
            landing.at[g], out.at[lane], send2.at[g], recv2.at[lane], (f, 2 * g + t // nf)
        )

    def own(g):
        return pltpu.make_async_copy(landing.at[g], out.at[lane], recv2.at[lane])

    def second_in(i):
        return remote(
            landing.at[0], out.at[i], send2.at[0], recv2.at[i], (f, t)
        )

    for j in range(nf):
        g = lax.rem(f + j, nf)
        if j:
            first_in(g).wait_recv()

        @pl.when(2 * g + t // nf != t)
        def _(g=g):
            second(g).start()

        @pl.when(2 * g + t // nf == t)
        def _(g=g):
            own(g).start()

    source = lax.rem(t, 2) * nf
    for i in range(nf):

        @pl.when(source + i != t)
        def _(i=i):
            second_in(i).wait_recv()

        @pl.when(source + i == t)
        def _(i=i):
            own(0).wait()

    for j in range(nf):
        g = lax.rem(f + j, nf)
        if j:
            first(g).wait_send()

        @pl.when(2 * g + t // nf != t)
        def _(g=g):
            second(g).wait_send()


def params(number):
    return pltpu.CompilerParams(
        collective_id=number, has_side_effects=True, vmem_limit_bytes=VMEM_LIMIT
    )


ANY = pl.BlockSpec(memory_space=pl.ANY)
VMEM = pl.BlockSpec(memory_space=pltpu.VMEM)
DMA = pltpu.SemaphoreType.DMA


def body(tokens, out_grad, gate_weight, up_weight, down_weight):
    nf, nt = lax.axis_size("fsdp"), lax.axis_size("tp")
    nz = nt // 2
    rows, shard = tokens.shape
    depth, width = gate_weight.shape
    count = rows * nf
    factor = 1.0 / math.sqrt(count)
    assert nt == 2 * nf and depth == 2 * shard

    pairs = jnp.concatenate([gate_weight, up_weight], axis=1)
    part = depth // nt
    whole, grads, turned = pl.pallas_call(
        functools.partial(spread_kernel, nf, nt),
        out_shape=(
            jax.ShapeDtypeStruct((count, depth), BF16),
            jax.ShapeDtypeStruct((count, depth), BF16),
            jax.ShapeDtypeStruct((part, nt * 2 * width), BF16),
        ),
        in_specs=[VMEM, VMEM, VMEM],
        out_specs=(VMEM, VMEM, VMEM),
        scratch_shapes=[
            pltpu.VMEM((2, nz, rows, shard), BF16),
            DMA((3,)),
            DMA((2, nz)),
            DMA((2, nz)),
            DMA((2, nz)),
            DMA((2, nz)),
            DMA((2, nf)),
            DMA((2, nf)),
            DMA((2, nf)),
            DMA((nt,)),
            DMA((nt,)),
        ],
        compiler_params=params(0),
        name="spread",
    )(tokens, out_grad, pairs)

    both = jnp.dot(whole, pairs, preferred_element_type=F32)
    back = lax.dot_general(
        grads, down_weight, (((1,), (1,)), ((), ())), preferred_element_type=F32
    )
    partial = jnp.concatenate([both, back], axis=1)

    deltas, hidden = pl.pallas_call(
        functools.partial(middle_kernel, nf, nt),
        out_shape=(
            jax.ShapeDtypeStruct((count, nt * 2 * width), BF16),
            jax.ShapeDtypeStruct((count, width), BF16),
        ),
        in_specs=[VMEM],
        out_specs=(VMEM, VMEM),
        scratch_shapes=[
            pltpu.VMEM((nf, rows, 3 * width), F32),
            pltpu.VMEM((1, nz, rows, 2 * width), BF16),
            pltpu.VMEM((rows, width), BF16),
            DMA((nf,)),
            DMA((nf,)),
            DMA((1, nz)),
            DMA((1, nz)),
            DMA((1, nz)),
            DMA((nz, nf)),
            DMA((nz, nf)),
            DMA((nz, nf)),
            DMA((nz, nf)),
            DMA((nf,)),
            DMA((nf,)),
            DMA((1,)),
        ],
        compiler_params=params(1),
        name="middle",
    )(partial)

    piece = lax.dot_general(
        deltas, turned, (((1,), (1,)), ((), ())), preferred_element_type=F32
    ).astype(BF16)
    input_grad = pl.pallas_call(
        functools.partial(return_kernel, nf, nt),
        out_shape=jax.ShapeDtypeStruct((nf, rows, part), BF16),
        in_specs=[VMEM],
        out_specs=VMEM,
        scratch_shapes=[
            pltpu.VMEM((nf, rows, part), BF16),
            DMA((nf,)),
            DMA((nf,)),
            DMA((nf,)),
            DMA((nf,)),
            DMA((1,)),
        ],
        compiler_params=params(2),
        name="back",
    )(piece)
    input_grad = input_grad.transpose(1, 0, 2).reshape(rows, shard)

    own = lax.dynamic_slice_in_dim(deltas, lax.axis_index("tp") * 2 * width, 2 * width, 1)
    contract = (((0,), (0,)), ((), ()))
    gate_grad = factor * lax.dot_general(
        whole, own[:, :width], contract, preferred_element_type=F32
    )
    up_grad = factor * lax.dot_general(
        whole, own[:, width:], contract, preferred_element_type=F32
    )
    down_grad = factor * lax.dot_general(hidden, grads, contract, preferred_element_type=F32)
    return (input_grad, gate_grad, up_grad, down_grad)


def solution(mesh):
    return jax.shard_map(
        body,
        mesh=mesh,
        in_specs=(
            P("fsdp", "tp"),
            P("fsdp", "tp"),
            P("fsdp", "tp"),
            P("fsdp", "tp"),
            P("tp", "fsdp"),
        ),
        out_specs=(P("fsdp", "tp"), P("fsdp", "tp"), P("fsdp", "tp"), P("tp", "fsdp")),
        check_vma=False,
    )
```

```python
import functools
import math

import jax
import jax.numpy as jnp
from jax import lax
from jax.sharding import PartitionSpec as P
from jax.experimental import pallas as pl
from jax.experimental.pallas import tpu as pltpu

MESH = pl.DeviceIdType.MESH
F32 = jnp.float32
BF16 = jnp.bfloat16
VMEM_LIMIT = 60 * 1024 * 1024


def place(nf, nt):
    return lax.axis_index("fsdp"), lax.axis_index("tp")


def enter(nf, nt):
    f, t = place(nf, nt)
    barrier = pltpu.get_barrier_semaphore()
    for j in range(1, nf):
        pl.semaphore_signal(
            barrier, inc=1, device_id=(lax.rem(f + j, nf), t), device_id_type=MESH
        )
    for j in range(1, nt):
        pl.semaphore_signal(
            barrier, inc=1, device_id=(f, lax.rem(t + j, nt)), device_id_type=MESH
        )
    pl.semaphore_wait(barrier, nf + nt - 2)


def remote(src, dst, send, recv, device):
    return pltpu.make_async_remote_copy(
        src_ref=src,
        dst_ref=dst,
        send_sem=send,
        recv_sem=recv,
        device_id=device,
        device_id_type=MESH,
    )


def line_steps(stage, mats, nz, f, t, up_send, down_send, recv, arrived):
    z = t // 2

    def up(m, b):
        return remote(
            stage.at[m, b], stage.at[m, b], up_send.at[m, b], recv.at[m, b], (f, t + 2)
        )

    def down(m, b):
        return remote(
            stage.at[m, b], stage.at[m, b], down_send.at[m, b], recv.at[m, b], (f, t - 2)
        )

    for s in range(nz):
        for m in range(mats):
            for direction in (0, 1) if s else (0,):
                b = z - s if direction == 0 else z + s

                @pl.when((b >= 0) & (b < nz))
                def _(m=m, b=b, s=s, direction=direction):
                    if s:
                        up(m, b).wait_recv()
                    if s == 0 or direction == 0:

                        @pl.when(z < nz - 1)
                        def _():
                            up(m, b).start()

                    if s == 0 or direction == 1:

                        @pl.when(z > 0)
                        def _():
                            down(m, b).start()

                    arrived(m, b)

    def finish():
        for b in range(nz):
            for m in range(mats):

                @pl.when((z < nz - 1) & (b <= z))
                def _(m=m, b=b):
                    up(m, b).wait_send()

                @pl.when((z > 0) & (b >= z))
                def _(m=m, b=b):
                    down(m, b).wait_send()

    return finish


def spread_kernel(
    nf,
    nt,
    tokens,
    grads,
    x_out,
    g_out,
    stage,
    local_sem,
    up_send,
    down_send,
    line_recv,
    plane_send,
    plane_recv,
    pair_send,
    pair_recv,
):
    f, t = place(nf, nt)
    nz = nt // 2
    z, k = t // 2, lax.rem(t, 2)
    rows, width = tokens.shape
    outs = (x_out, g_out)
    loads = []
    for m, ref in enumerate((tokens, grads)):
        load = pltpu.make_async_copy(ref, stage.at[m, z], local_sem.at[m])
        load.start()
        loads.append(load)
    enter(nf, nt)
    for load in loads:
        load.wait()

    half = pl.ds(pl.multiple_of(k * width, width), width)

    def spot(m, g):
        return outs[m].at[pl.ds(pl.multiple_of(g * rows, rows), rows), half]

    def plane(m, b):
        return remote(
            stage.at[m, b], spot(m, f), plane_send.at[m, b], plane_recv.at[m, f], (b, t)
        )

    def plane_in(m, g):
        return remote(
            stage.at[m, 0], spot(m, g), plane_send.at[m, 0], plane_recv.at[m, g], (f, t)
        )

    def keep(m):
        return pltpu.make_async_copy(stage.at[m, f], spot(m, f), plane_recv.at[m, f])

    def arrived(m, b):
        @pl.when(b != f)
        def _():
            plane(m, b).start()

        @pl.when(b == f)
        def _():
            keep(m).start()

    finish = line_steps(
        stage, 2, nz, f, t, up_send, down_send, line_recv, arrived
    )

    def pair(m, g):
        return remote(
            spot(m, g), spot(m, g), pair_send.at[m, g], pair_recv.at[m, g], (f, t + 1 - 2 * k)
        )

    for m in range(2):
        for j in range(nf):
            g = lax.rem(f + j, nf)
            if j == 0:
                keep(m).wait()
            else:
                plane_in(m, g).wait_recv()
            pair(m, g).start()
    finish()
    for m in range(2):
        for b in range(nz):

            @pl.when(b != f)
            def _(m=m, b=b):
                plane(m, b).wait_send()

        for g in range(nf):
            pair(m, g).wait()


def middle_kernel(
    nf,
    nt,
    partial,
    weights,
    all_out,
    hidden_out,
    w_out,
    landing,
    stage,
    hidden_own,
    sum_send,
    sum_recv,
    up_send,
    down_send,
    line_recv,
    plane_send,
    plane_recv,
    pair_send,
    pair_recv,
    h_send,
    h_recv,
    local_sem,
    w_send,
    w_recv,
):
    f, t = place(nf, nt)
    nz = nt // 2
    z, k = t // 2, lax.rem(t, 2)
    rows = landing.shape[1]
    width = hidden_own.shape[1]

    def block(g):
        return pl.ds(pl.multiple_of(g * rows, rows), rows)

    part = w_out.shape[0]
    depth = weights.shape[1]
    w_own = pltpu.make_async_copy(
        weights.at[pl.ds(t * part, part)],
        w_out.at[:, pl.ds(pl.multiple_of(t * depth, depth), depth)],
        local_sem.at[1],
    )
    w_own.start()
    enter(nf, nt)

    def share(g):
        return remote(
            partial.at[block(g)], landing.at[f], sum_send.at[g], sum_recv.at[f], (g, t)
        )

    def share_in(g):
        return remote(
            partial.at[block(g)], landing.at[g], sum_send.at[g], sum_recv.at[g], (g, t)
        )

    for j in range(1, nf):
        share(lax.rem(f + j, nf)).start()

    def w_copy(u):
        return remote(
            weights.at[pl.ds(u * part, part)],
            w_out.at[:, pl.ds(pl.multiple_of(t * depth, depth), depth)],
            w_send.at[u],
            w_recv.at[t],
            (f, u),
        )

    def w_in(u):
        return remote(
            weights.at[pl.ds(0, part)],
            w_out.at[:, pl.ds(pl.multiple_of(u * depth, depth), depth)],
            w_send.at[u],
            w_recv.at[u],
            (f, u),
        )

    for j in range(1, nt):
        w_copy(lax.rem(t + j, nt)).start()

    for j in range(1, nf):
        share_in(lax.rem(f + j, nf)).wait_recv()
    total = partial[block(f), :]
    for j in range(1, nf):
        total = total + landing[lax.rem(f + j, nf)]
    gate = total[:, :width]
    up = total[:, width : 2 * width]
    hidden_grad = total[:, 2 * width :]
    squashed = jax.nn.sigmoid(gate)
    activated = gate * squashed
    slope = squashed * (1.0 + gate * (1.0 - squashed))
    stage[0, z, :, :width] = (hidden_grad * up * slope).astype(BF16)
    stage[0, z, :, width:] = (hidden_grad * activated).astype(BF16)
    hidden_own[...] = (activated * up).astype(BF16)

    def h_copy(g):
        return remote(
            hidden_own, hidden_out.at[block(f)], h_send.at[g], h_recv.at[f], (g, t)
        )

    def h_in(g):
        return remote(
            hidden_own, hidden_out.at[block(g)], h_send.at[g], h_recv.at[g], (g, t)
        )

    def spot(g, b):
        at = pl.multiple_of((2 * b + k) * 2 * width, 2 * width)
        return all_out.at[block(g), pl.ds(at, 2 * width)]

    def plane(b, g):
        return remote(
            stage.at[0, b], spot(f, b), plane_send.at[b, g], plane_recv.at[b, f], (g, t)
        )

    def plane_in(b, g):
        return remote(
            stage.at[0, b], spot(g, b), plane_send.at[b, g], plane_recv.at[b, g], (g, t)
        )

    def keep(b):
        return pltpu.make_async_copy(stage.at[0, b], spot(f, b), plane_recv.at[b, f])

    def arrived(m, b):
        for j in range(1, nf):
            plane(b, lax.rem(f + j, nf)).start()
        keep(b).start()

    finish = line_steps(stage, 1, nz, f, t, up_send, down_send, line_recv, arrived)
    for j in range(1, nf):
        h_copy(lax.rem(f + j, nf)).start()
    h_keep = pltpu.make_async_copy(hidden_own, hidden_out.at[block(f)], local_sem.at[0])
    h_keep.start()

    def pair(b, g):
        return remote(
            spot(g, b), spot(g, b), pair_send.at[b, g], pair_recv.at[b, g], (f, t + 1 - 2 * k)
        )

    def pair_in(b, g):
        at = pl.multiple_of((2 * b + 1 - k) * 2 * width, 2 * width)
        here = all_out.at[block(g), pl.ds(at, 2 * width)]
        return remote(
            here, here, pair_send.at[b, g], pair_recv.at[b, g], (f, t + 1 - 2 * k)
        )

    for b in range(nz):
        for j in range(nf):
            g = lax.rem(f + j, nf)
            if j == 0:
                keep(b).wait()
            else:
                plane_in(b, g).wait_recv()
            pair(b, g).start()
    finish()
    h_keep.wait()
    for j in range(1, nf):
        g = lax.rem(f + j, nf)
        share(g).wait_send()
        h_copy(g).wait_send()
        h_in(g).wait_recv()
        for b in range(nz):
            plane(b, g).wait_send()
    for b in range(nz):
        for g in range(nf):
            pair(b, g).wait_send()
            pair_in(b, g).wait_recv()
    w_own.wait()
    for j in range(1, nt):
        u = lax.rem(t + j, nt)
        w_copy(u).wait_send()
        w_in(u).wait_recv()


def return_kernel(nf, nt, result, out, landing, send, recv, send2, recv2, local_sem):
    f, t = place(nf, nt)
    rows = landing.shape[1]

    def block(g):
        return pl.ds(pl.multiple_of(g * rows, rows), rows)

    keep = pltpu.make_async_copy(result.at[block(f)], landing.at[f], local_sem.at[0])
    keep.start()
    enter(nf, nt)

    def first(g):
        return remote(result.at[block(g)], landing.at[f], send.at[g], recv.at[f], (g, t))

    def first_in(g):
        return remote(result.at[block(g)], landing.at[g], send.at[g], recv.at[g], (g, t))

    for j in range(1, nf):
        first(lax.rem(f + j, nf)).start()
    keep.wait()
    lane = lax.rem(t, nf)

    def second(g):
        return remote(
            landing.at[g], out.at[lane], send2.at[g], recv2.at[lane], (f, 2 * g + t // nf)
        )

    def own(g):
        return pltpu.make_async_copy(landing.at[g], out.at[lane], recv2.at[lane])

    def second_in(i):
        return remote(
            landing.at[0], out.at[i], send2.at[0], recv2.at[i], (f, t)
        )

    for j in range(nf):
        g = lax.rem(f + j, nf)
        if j:
            first_in(g).wait_recv()

        @pl.when(2 * g + t // nf != t)
        def _(g=g):
            second(g).start()

        @pl.when(2 * g + t // nf == t)
        def _(g=g):
            own(g).start()

    source = lax.rem(t, 2) * nf
    for i in range(nf):

        @pl.when(source + i != t)
        def _(i=i):
            second_in(i).wait_recv()

        @pl.when(source + i == t)
        def _(i=i):
            own(0).wait()

    for j in range(nf):
        g = lax.rem(f + j, nf)
        if j:
            first(g).wait_send()

        @pl.when(2 * g + t // nf != t)
        def _(g=g):
            second(g).wait_send()


def params(number):
    return pltpu.CompilerParams(
        collective_id=number, has_side_effects=True, vmem_limit_bytes=VMEM_LIMIT
    )


ANY = pl.BlockSpec(memory_space=pl.ANY)
VMEM = pl.BlockSpec(memory_space=pltpu.VMEM)
DMA = pltpu.SemaphoreType.DMA


def body(tokens, out_grad, gate_weight, up_weight, down_weight):
    nf, nt = lax.axis_size("fsdp"), lax.axis_size("tp")
    nz = nt // 2
    rows, shard = tokens.shape
    depth, width = gate_weight.shape
    count = rows * nf
    factor = 1.0 / math.sqrt(count)
    assert nt == 2 * nf and depth == 2 * shard

    pairs = jnp.concatenate([gate_weight, up_weight], axis=1)
    part = depth // nt
    whole, grads = pl.pallas_call(
        functools.partial(spread_kernel, nf, nt),
        out_shape=(
            jax.ShapeDtypeStruct((count, depth), BF16),
            jax.ShapeDtypeStruct((count, depth), BF16),
        ),
        in_specs=[VMEM, VMEM],
        out_specs=(VMEM, VMEM),
        scratch_shapes=[
            pltpu.VMEM((2, nz, rows, shard), BF16),
            DMA((2,)),
            DMA((2, nz)),
            DMA((2, nz)),
            DMA((2, nz)),
            DMA((2, nz)),
            DMA((2, nf)),
            DMA((2, nf)),
            DMA((2, nf)),
        ],
        compiler_params=params(0),
        name="spread",
    )(tokens, out_grad)

    both = jnp.dot(whole, pairs, preferred_element_type=F32)
    back = lax.dot_general(
        grads, down_weight, (((1,), (1,)), ((), ())), preferred_element_type=F32
    )
    partial = jnp.concatenate([both, back], axis=1)

    deltas, hidden, turned = pl.pallas_call(
        functools.partial(middle_kernel, nf, nt),
        out_shape=(
            jax.ShapeDtypeStruct((count, nt * 2 * width), BF16),
            jax.ShapeDtypeStruct((count, width), BF16),
            jax.ShapeDtypeStruct((part, nt * 2 * width), BF16),
        ),
        in_specs=[VMEM, VMEM],
        out_specs=(VMEM, VMEM, VMEM),
        scratch_shapes=[
            pltpu.VMEM((nf, rows, 3 * width), F32),
            pltpu.VMEM((1, nz, rows, 2 * width), BF16),
            pltpu.VMEM((rows, width), BF16),
            DMA((nf,)),
            DMA((nf,)),
            DMA((1, nz)),
            DMA((1, nz)),
            DMA((1, nz)),
            DMA((nz, nf)),
            DMA((nz, nf)),
            DMA((nz, nf)),
            DMA((nz, nf)),
            DMA((nf,)),
            DMA((nf,)),
            DMA((2,)),
            DMA((nt,)),
            DMA((nt,)),
        ],
        compiler_params=params(1),
        name="middle",
    )(partial, pairs)

    piece = lax.dot_general(
        deltas, turned, (((1,), (1,)), ((), ())), preferred_element_type=F32
    ).astype(BF16)
    input_grad = pl.pallas_call(
        functools.partial(return_kernel, nf, nt),
        out_shape=jax.ShapeDtypeStruct((nf, rows, part), BF16),
        in_specs=[VMEM],
        out_specs=VMEM,
        scratch_shapes=[
            pltpu.VMEM((nf, rows, part), BF16),
            DMA((nf,)),
            DMA((nf,)),
            DMA((nf,)),
            DMA((nf,)),
            DMA((1,)),
        ],
        compiler_params=params(2),
        name="back",
    )(piece)
    input_grad = input_grad.transpose(1, 0, 2).reshape(rows, shard)

    own = lax.dynamic_slice_in_dim(deltas, lax.axis_index("tp") * 2 * width, 2 * width, 1)
    contract = (((0,), (0,)), ((), ()))
    gate_grad = factor * lax.dot_general(
        whole, own[:, :width], contract, preferred_element_type=F32
    )
    up_grad = factor * lax.dot_general(
        whole, own[:, width:], contract, preferred_element_type=F32
    )
    down_grad = factor * lax.dot_general(hidden, grads, contract, preferred_element_type=F32)
    return (input_grad, gate_grad, up_grad, down_grad)


def solution(mesh):
    return jax.shard_map(
        body,
        mesh=mesh,
        in_specs=(
            P("fsdp", "tp"),
            P("fsdp", "tp"),
            P("fsdp", "tp"),
            P("fsdp", "tp"),
            P("tp", "fsdp"),
        ),
        out_specs=(P("fsdp", "tp"), P("fsdp", "tp"), P("fsdp", "tp"), P("tp", "fsdp")),
        check_vma=False,
    )
```

```python
import functools
import math

import jax
import jax.numpy as jnp
from jax import lax
from jax.sharding import PartitionSpec as P
from jax.experimental import pallas as pl
from jax.experimental.pallas import tpu as pltpu

MESH = pl.DeviceIdType.MESH
F32 = jnp.float32
BF16 = jnp.bfloat16
VMEM_LIMIT = 60 * 1024 * 1024
CHUNKS = 4
AHEAD = 2


def place(nf, nt):
    return lax.axis_index("fsdp"), lax.axis_index("tp")


def enter(nf, nt):
    f, t = place(nf, nt)
    barrier = pltpu.get_barrier_semaphore()
    for j in range(1, nf):
        pl.semaphore_signal(
            barrier, inc=1, device_id=(lax.rem(f + j, nf), t), device_id_type=MESH
        )
    for j in range(1, nt):
        pl.semaphore_signal(
            barrier, inc=1, device_id=(f, lax.rem(t + j, nt)), device_id_type=MESH
        )
    pl.semaphore_wait(barrier, nf + nt - 2)


def remote(src, dst, send, recv, device):
    return pltpu.make_async_remote_copy(
        src_ref=src,
        dst_ref=dst,
        send_sem=send,
        recv_sem=recv,
        device_id=device,
        device_id_type=MESH,
    )


def line_steps(stage, mats, nz, f, t, up_send, down_send, recv, arrived):
    z = t // 2

    def up(m, b):
        return remote(
            stage.at[m, b], stage.at[m, b], up_send.at[m, b], recv.at[m, b], (f, t + 2)
        )

    def down(m, b):
        return remote(
            stage.at[m, b], stage.at[m, b], down_send.at[m, b], recv.at[m, b], (f, t - 2)
        )

    for s in range(nz):
        for m in range(mats):
            for direction in (0, 1) if s else (0,):
                b = z - s if direction == 0 else z + s

                @pl.when((b >= 0) & (b < nz))
                def _(m=m, b=b, s=s, direction=direction):
                    if s:
                        up(m, b).wait_recv()
                    if s == 0 or direction == 0:

                        @pl.when(z < nz - 1)
                        def _():
                            up(m, b).start()

                    if s == 0 or direction == 1:

                        @pl.when(z > 0)
                        def _():
                            down(m, b).start()

                    arrived(m, b)

    def finish():
        for b in range(nz):
            for m in range(mats):

                @pl.when((z < nz - 1) & (b <= z))
                def _(m=m, b=b):
                    up(m, b).wait_send()

                @pl.when((z > 0) & (b >= z))
                def _(m=m, b=b):
                    down(m, b).wait_send()

    return finish


def spread_kernel(
    nf,
    nt,
    tokens,
    grads,
    x_out,
    g_out,
    stage,
    local_sem,
    up_send,
    down_send,
    line_recv,
    plane_send,
    plane_recv,
    pair_send,
    pair_recv,
):
    f, t = place(nf, nt)
    nz = nt // 2
    z, k = t // 2, lax.rem(t, 2)
    rows, width = tokens.shape
    size = rows // CHUNKS
    outs = (x_out, g_out)
    loads = []
    for m, ref in enumerate((tokens, grads)):
        load = pltpu.make_async_copy(ref, stage.at[m, z], local_sem.at[m])
        load.start()
        loads.append(load)
    enter(nf, nt)
    for load in loads:
        load.wait()

    half = pl.ds(pl.multiple_of(k * width, width), width)

    def held(m, b, c):
        return stage.at[m, b, pl.ds(c * size, size)]

    def spot(m, g, c):
        return outs[m].at[pl.ds(pl.multiple_of(g * rows + c * size, size), size), half]

    def up(m, b, c):
        here = held(m, b, c)
        return remote(here, here, up_send.at[m, b, c], line_recv.at[m, b, c], (f, t + 2))

    def down(m, b, c):
        here = held(m, b, c)
        return remote(here, here, down_send.at[m, b, c], line_recv.at[m, b, c], (f, t - 2))

    def plane(m, b, c):
        return remote(
            held(m, b, c), spot(m, f, c), plane_send.at[m, b, c], plane_recv.at[m, f, c], (b, t)
        )

    def plane_in(m, g, c):
        return remote(
            held(m, 0, c), spot(m, g, c), plane_send.at[m, 0, c], plane_recv.at[m, g, c], (f, t)
        )

    def keep(m, c):
        return pltpu.make_async_copy(held(m, f, c), spot(m, f, c), plane_recv.at[m, f, c])

    def arrived(m, b, c):
        @pl.when(b != f)
        def _():
            plane(m, b, c).start()

        @pl.when(b == f)
        def _():
            keep(m, c).start()

    def send_own(c):
        for m in range(2):

            @pl.when(z < nz - 1)
            def _(m=m):
                up(m, z, c).start()

            @pl.when(z > 0)
            def _(m=m):
                down(m, z, c).start()

    def pair(m, g, c):
        here = spot(m, g, c)
        return remote(
            here, here, pair_send.at[m, g, c], pair_recv.at[m, g, c], (f, t + 1 - 2 * k)
        )

    def swap(c):
        for m in range(2):
            for j in range(nf):
                g = lax.rem(f + j, nf)
                if j == 0:
                    keep(m, c).wait()
                else:
                    plane_in(m, g, c).wait_recv()
                pair(m, g, c).start()

    edge = (z == 0) | (z == nz - 1)
    for c in range(CHUNKS):
        if c < AHEAD:
            send_own(c)
        else:

            @pl.when(edge)
            def _(c=c):
                send_own(c)

    for c in range(CHUNKS):
        for m in range(2):
            arrived(m, z, c)
        for s in range(1, nz):
            for direction in (0, 1):
                b = z - s if direction == 0 else z + s

                @pl.when((b >= 0) & (b < nz))
                def _(b=b, direction=direction):
                    for m in range(2):
                        up(m, b, c).wait_recv()
                        if direction == 0:

                            @pl.when(z < nz - 1)
                            def _():
                                up(m, b, c).start()

                        else:

                            @pl.when(z > 0)
                            def _():
                                down(m, b, c).start()

                        arrived(m, b, c)

        if c + AHEAD < CHUNKS:

            @pl.when(jnp.logical_not(edge))
            def _(c=c):
                send_own(c + AHEAD)

        if c >= 2:
            swap(c - 2)
    for c in range(max(CHUNKS - 2, 0), CHUNKS):
        swap(c)
    for c in range(CHUNKS):
        for m in range(2):
            for b in range(nz):

                @pl.when((z < nz - 1) & (b <= z))
                def _(m=m, b=b):
                    up(m, b, c).wait_send()

                @pl.when((z > 0) & (b >= z))
                def _(m=m, b=b):
                    down(m, b, c).wait_send()

                @pl.when(b != f)
                def _(m=m, b=b):
                    plane(m, b, c).wait_send()

            for g in range(nf):
                pair(m, g, c).wait()


def middle_kernel(
    nf,
    nt,
    partial,
    weights,
    all_out,
    hidden_out,
    w_out,
    landing,
    stage,
    hidden_own,
    sum_send,
    sum_recv,
    up_send,
    down_send,
    line_recv,
    plane_send,
    plane_recv,
    pair_send,
    pair_recv,
    h_send,
    h_recv,
    local_sem,
    w_send,
    w_recv,
):
    f, t = place(nf, nt)
    nz = nt // 2
    z, k = t // 2, lax.rem(t, 2)
    rows = landing.shape[1]
    width = hidden_own.shape[1]

    def block(g):
        return pl.ds(pl.multiple_of(g * rows, rows), rows)

    part = w_out.shape[0]
    depth = weights.shape[1]
    w_own = pltpu.make_async_copy(
        weights.at[pl.ds(t * part, part)],
        w_out.at[:, pl.ds(pl.multiple_of(t * depth, depth), depth)],
        local_sem.at[1],
    )
    w_own.start()
    enter(nf, nt)

    def share(g):
        return remote(
            partial.at[block(g)], landing.at[f], sum_send.at[g], sum_recv.at[f], (g, t)
        )

    def share_in(g):
        return remote(
            partial.at[block(g)], landing.at[g], sum_send.at[g], sum_recv.at[g], (g, t)
        )

    for j in range(1, nf):
        share(lax.rem(f + j, nf)).start()

    def w_copy(u):
        return remote(
            weights.at[pl.ds(u * part, part)],
            w_out.at[:, pl.ds(pl.multiple_of(t * depth, depth), depth)],
            w_send.at[u],
            w_recv.at[t],
            (f, u),
        )

    def w_in(u):
        return remote(
            weights.at[pl.ds(0, part)],
            w_out.at[:, pl.ds(pl.multiple_of(u * depth, depth), depth)],
            w_send.at[u],
            w_recv.at[u],
            (f, u),
        )

    for j in range(1, nt):
        w_copy(lax.rem(t + j, nt)).start()

    for j in range(1, nf):
        share_in(lax.rem(f + j, nf)).wait_recv()
    total = partial[block(f), :]
    for j in range(1, nf):
        total = total + landing[lax.rem(f + j, nf)]
    gate = total[:, :width]
    up = total[:, width : 2 * width]
    hidden_grad = total[:, 2 * width :]
    squashed = jax.nn.sigmoid(gate)
    activated = gate * squashed
    slope = squashed * (1.0 + gate * (1.0 - squashed))
    stage[0, z, :, :width] = (hidden_grad * up * slope).astype(BF16)
    stage[0, z, :, width:] = (hidden_grad * activated).astype(BF16)
    hidden_own[...] = (activated * up).astype(BF16)

    def h_copy(g):
        return remote(
            hidden_own, hidden_out.at[block(f)], h_send.at[g], h_recv.at[f], (g, t)
        )

    def h_in(g):
        return remote(
            hidden_own, hidden_out.at[block(g)], h_send.at[g], h_recv.at[g], (g, t)
        )

    def spot(g, b):
        at = pl.multiple_of((2 * b + k) * 2 * width, 2 * width)
        return all_out.at[block(g), pl.ds(at, 2 * width)]

    def plane(b, g):
        return remote(
            stage.at[0, b], spot(f, b), plane_send.at[b, g], plane_recv.at[b, f], (g, t)
        )

    def plane_in(b, g):
        return remote(
            stage.at[0, b], spot(g, b), plane_send.at[b, g], plane_recv.at[b, g], (g, t)
        )

    def keep(b):
        return pltpu.make_async_copy(stage.at[0, b], spot(f, b), plane_recv.at[b, f])

    def arrived(m, b):
        for j in range(1, nf):
            plane(b, lax.rem(f + j, nf)).start()
        keep(b).start()

    finish = line_steps(stage, 1, nz, f, t, up_send, down_send, line_recv, arrived)
    for j in range(1, nf):
        h_copy(lax.rem(f + j, nf)).start()
    h_keep = pltpu.make_async_copy(hidden_own, hidden_out.at[block(f)], local_sem.at[0])
    h_keep.start()

    def pair(b, g):
        return remote(
            spot(g, b), spot(g, b), pair_send.at[b, g], pair_recv.at[b, g], (f, t + 1 - 2 * k)
        )

    def pair_in(b, g):
        at = pl.multiple_of((2 * b + 1 - k) * 2 * width, 2 * width)
        here = all_out.at[block(g), pl.ds(at, 2 * width)]
        return remote(
            here, here, pair_send.at[b, g], pair_recv.at[b, g], (f, t + 1 - 2 * k)
        )

    for b in range(nz):
        for j in range(nf):
            g = lax.rem(f + j, nf)
            if j == 0:
                keep(b).wait()
            else:
                plane_in(b, g).wait_recv()
            pair(b, g).start()
    finish()
    h_keep.wait()
    for j in range(1, nf):
        g = lax.rem(f + j, nf)
        share(g).wait_send()
        h_copy(g).wait_send()
        h_in(g).wait_recv()
        for b in range(nz):
            plane(b, g).wait_send()
    for b in range(nz):
        for g in range(nf):
            pair(b, g).wait_send()
            pair_in(b, g).wait_recv()
    w_own.wait()
    for j in range(1, nt):
        u = lax.rem(t + j, nt)
        w_copy(u).wait_send()
        w_in(u).wait_recv()


def return_kernel(nf, nt, result, out, landing, send, recv, send2, recv2, local_sem):
    f, t = place(nf, nt)
    rows = landing.shape[1]

    def block(g):
        return pl.ds(pl.multiple_of(g * rows, rows), rows)

    keep = pltpu.make_async_copy(result.at[block(f)], landing.at[f], local_sem.at[0])
    keep.start()
    enter(nf, nt)

    def first(g):
        return remote(result.at[block(g)], landing.at[f], send.at[g], recv.at[f], (g, t))

    def first_in(g):
        return remote(result.at[block(g)], landing.at[g], send.at[g], recv.at[g], (g, t))

    for j in range(1, nf):
        first(lax.rem(f + j, nf)).start()
    keep.wait()
    lane = lax.rem(t, nf)

    def second(g):
        return remote(
            landing.at[g], out.at[lane], send2.at[g], recv2.at[lane], (f, 2 * g + t // nf)
        )

    def own(g):
        return pltpu.make_async_copy(landing.at[g], out.at[lane], recv2.at[lane])

    def second_in(i):
        return remote(
            landing.at[0], out.at[i], send2.at[0], recv2.at[i], (f, t)
        )

    for j in range(nf):
        g = lax.rem(f + j, nf)
        if j:
            first_in(g).wait_recv()

        @pl.when(2 * g + t // nf != t)
        def _(g=g):
            second(g).start()

        @pl.when(2 * g + t // nf == t)
        def _(g=g):
            own(g).start()

    source = lax.rem(t, 2) * nf
    for i in range(nf):

        @pl.when(source + i != t)
        def _(i=i):
            second_in(i).wait_recv()

        @pl.when(source + i == t)
        def _(i=i):
            own(0).wait()

    for j in range(nf):
        g = lax.rem(f + j, nf)
        if j:
            first(g).wait_send()

        @pl.when(2 * g + t // nf != t)
        def _(g=g):
            second(g).wait_send()


def params(number):
    return pltpu.CompilerParams(
        collective_id=number, has_side_effects=True, vmem_limit_bytes=VMEM_LIMIT
    )


ANY = pl.BlockSpec(memory_space=pl.ANY)
VMEM = pl.BlockSpec(memory_space=pltpu.VMEM)
DMA = pltpu.SemaphoreType.DMA


def body(tokens, out_grad, gate_weight, up_weight, down_weight):
    nf, nt = lax.axis_size("fsdp"), lax.axis_size("tp")
    nz = nt // 2
    rows, shard = tokens.shape
    depth, width = gate_weight.shape
    count = rows * nf
    factor = 1.0 / math.sqrt(count)
    assert nt == 2 * nf and depth == 2 * shard

    pairs = jnp.concatenate([gate_weight, up_weight], axis=1)
    part = depth // nt
    whole, grads = pl.pallas_call(
        functools.partial(spread_kernel, nf, nt),
        out_shape=(
            jax.ShapeDtypeStruct((count, depth), BF16),
            jax.ShapeDtypeStruct((count, depth), BF16),
        ),
        in_specs=[VMEM, VMEM],
        out_specs=(VMEM, VMEM),
        scratch_shapes=[
            pltpu.VMEM((2, nz, rows, shard), BF16),
            DMA((2,)),
            DMA((2, nz, CHUNKS)),
            DMA((2, nz, CHUNKS)),
            DMA((2, nz, CHUNKS)),
            DMA((2, nz, CHUNKS)),
            DMA((2, nf, CHUNKS)),
            DMA((2, nf, CHUNKS)),
            DMA((2, nf, CHUNKS)),
        ],
        compiler_params=params(0),
        name="spread",
    )(tokens, out_grad)

    both = jnp.dot(whole, pairs, preferred_element_type=F32)
    back = lax.dot_general(
        grads, down_weight, (((1,), (1,)), ((), ())), preferred_element_type=F32
    )
    partial = jnp.concatenate([both, back], axis=1)

    deltas, hidden, turned = pl.pallas_call(
        functools.partial(middle_kernel, nf, nt),
        out_shape=(
            jax.ShapeDtypeStruct((count, nt * 2 * width), BF16),
            jax.ShapeDtypeStruct((count, width), BF16),
            jax.ShapeDtypeStruct((part, nt * 2 * width), BF16),
        ),
        in_specs=[VMEM, VMEM],
        out_specs=(VMEM, VMEM, VMEM),
        scratch_shapes=[
            pltpu.VMEM((nf, rows, 3 * width), F32),
            pltpu.VMEM((1, nz, rows, 2 * width), BF16),
            pltpu.VMEM((rows, width), BF16),
            DMA((nf,)),
            DMA((nf,)),
            DMA((1, nz)),
            DMA((1, nz)),
            DMA((1, nz)),
            DMA((nz, nf)),
            DMA((nz, nf)),
            DMA((nz, nf)),
            DMA((nz, nf)),
            DMA((nf,)),
            DMA((nf,)),
            DMA((2,)),
            DMA((nt,)),
            DMA((nt,)),
        ],
        compiler_params=params(1),
        name="middle",
    )(partial, pairs)

    piece = lax.dot_general(
        deltas, turned, (((1,), (1,)), ((), ())), preferred_element_type=F32
    ).astype(BF16)
    input_grad = pl.pallas_call(
        functools.partial(return_kernel, nf, nt),
        out_shape=jax.ShapeDtypeStruct((nf, rows, part), BF16),
        in_specs=[VMEM],
        out_specs=VMEM,
        scratch_shapes=[
            pltpu.VMEM((nf, rows, part), BF16),
            DMA((nf,)),
            DMA((nf,)),
            DMA((nf,)),
            DMA((nf,)),
            DMA((1,)),
        ],
        compiler_params=params(2),
        name="back",
    )(piece)
    input_grad = input_grad.transpose(1, 0, 2).reshape(rows, shard)

    own = lax.dynamic_slice_in_dim(deltas, lax.axis_index("tp") * 2 * width, 2 * width, 1)
    contract = (((0,), (0,)), ((), ()))
    gate_grad = factor * lax.dot_general(
        whole, own[:, :width], contract, preferred_element_type=F32
    )
    up_grad = factor * lax.dot_general(
        whole, own[:, width:], contract, preferred_element_type=F32
    )
    down_grad = factor * lax.dot_general(hidden, grads, contract, preferred_element_type=F32)
    return (input_grad, gate_grad, up_grad, down_grad)


def solution(mesh):
    return jax.shard_map(
        body,
        mesh=mesh,
        in_specs=(
            P("fsdp", "tp"),
            P("fsdp", "tp"),
            P("fsdp", "tp"),
            P("fsdp", "tp"),
            P("tp", "fsdp"),
        ),
        out_specs=(P("fsdp", "tp"), P("fsdp", "tp"), P("fsdp", "tp"), P("tp", "fsdp")),
        check_vma=False,
    )
```

```python
import functools
import math

import jax
import jax.numpy as jnp
from jax import lax
from jax.sharding import PartitionSpec as P
from jax.experimental import pallas as pl
from jax.experimental.pallas import tpu as pltpu

MESH = pl.DeviceIdType.MESH
F32 = jnp.float32
BF16 = jnp.bfloat16
VMEM_LIMIT = 60 * 1024 * 1024
CHUNKS = 4
AHEAD = 2
TILE = 512


def place(nf, nt):
    return lax.axis_index("fsdp"), lax.axis_index("tp")


def enter(nf, nt):
    f, t = place(nf, nt)
    barrier = pltpu.get_barrier_semaphore()
    for j in range(1, nf):
        pl.semaphore_signal(
            barrier, inc=1, device_id=(lax.rem(f + j, nf), t), device_id_type=MESH
        )
    for j in range(1, nt):
        pl.semaphore_signal(
            barrier, inc=1, device_id=(f, lax.rem(t + j, nt)), device_id_type=MESH
        )
    pl.semaphore_wait(barrier, nf + nt - 2)


def remote(src, dst, send, recv, device):
    return pltpu.make_async_remote_copy(
        src_ref=src,
        dst_ref=dst,
        send_sem=send,
        recv_sem=recv,
        device_id=device,
        device_id_type=MESH,
    )


def line_steps(stage, mats, nz, f, t, up_send, down_send, recv, arrived):
    z = t // 2

    def up(m, b):
        return remote(
            stage.at[m, b], stage.at[m, b], up_send.at[m, b], recv.at[m, b], (f, t + 2)
        )

    def down(m, b):
        return remote(
            stage.at[m, b], stage.at[m, b], down_send.at[m, b], recv.at[m, b], (f, t - 2)
        )

    for s in range(nz):
        for m in range(mats):
            for direction in (0, 1) if s else (0,):
                b = z - s if direction == 0 else z + s

                @pl.when((b >= 0) & (b < nz))
                def _(m=m, b=b, s=s, direction=direction):
                    if s:
                        up(m, b).wait_recv()
                    if s == 0 or direction == 0:

                        @pl.when(z < nz - 1)
                        def _():
                            up(m, b).start()

                    if s == 0 or direction == 1:

                        @pl.when(z > 0)
                        def _():
                            down(m, b).start()

                    arrived(m, b)

    def finish():
        for b in range(nz):
            for m in range(mats):

                @pl.when((z < nz - 1) & (b <= z))
                def _(m=m, b=b):
                    up(m, b).wait_send()

                @pl.when((z > 0) & (b >= z))
                def _(m=m, b=b):
                    down(m, b).wait_send()

    return finish


def spread_kernel(
    nf,
    nt,
    tokens,
    grads,
    x_out,
    g_out,
    stage,
    local_sem,
    up_send,
    down_send,
    line_recv,
    plane_send,
    plane_recv,
    pair_send,
    pair_recv,
):
    f, t = place(nf, nt)
    nz = nt // 2
    z, k = t // 2, lax.rem(t, 2)
    rows, width = tokens.shape
    size = rows // CHUNKS
    outs = (x_out, g_out)
    loads = []
    for m, ref in enumerate((tokens, grads)):
        load = pltpu.make_async_copy(ref, stage.at[m, z], local_sem.at[m])
        load.start()
        loads.append(load)
    enter(nf, nt)
    for load in loads:
        load.wait()

    half = pl.ds(pl.multiple_of(k * width, width), width)

    def held(m, b, c):
        return stage.at[m, b, pl.ds(c * size, size)]

    def spot(m, g, c):
        return outs[m].at[pl.ds(pl.multiple_of(g * rows + c * size, size), size), half]

    def up(m, b, c):
        here = held(m, b, c)
        return remote(here, here, up_send.at[m, b, c], line_recv.at[m, b, c], (f, t + 2))

    def down(m, b, c):
        here = held(m, b, c)
        return remote(here, here, down_send.at[m, b, c], line_recv.at[m, b, c], (f, t - 2))

    def plane(m, b, c):
        return remote(
            held(m, b, c), spot(m, f, c), plane_send.at[m, b, c], plane_recv.at[m, f, c], (b, t)
        )

    def plane_in(m, g, c):
        return remote(
            held(m, 0, c), spot(m, g, c), plane_send.at[m, 0, c], plane_recv.at[m, g, c], (f, t)
        )

    def keep(m, c):
        return pltpu.make_async_copy(held(m, f, c), spot(m, f, c), plane_recv.at[m, f, c])

    def arrived(m, b, c):
        @pl.when(b != f)
        def _():
            plane(m, b, c).start()

        @pl.when(b == f)
        def _():
            keep(m, c).start()

    def send_own(c):
        for m in range(2):

            @pl.when(z < nz - 1)
            def _(m=m):
                up(m, z, c).start()

            @pl.when(z > 0)
            def _(m=m):
                down(m, z, c).start()

    def pair(m, g, c):
        here = spot(m, g, c)
        return remote(
            here, here, pair_send.at[m, g, c], pair_recv.at[m, g, c], (f, t + 1 - 2 * k)
        )

    def swap(c):
        for m in range(2):
            for j in range(nf):
                g = lax.rem(f + j, nf)
                if j == 0:
                    keep(m, c).wait()
                else:
                    plane_in(m, g, c).wait_recv()
                pair(m, g, c).start()

    edge = (z == 0) | (z == nz - 1)
    for c in range(CHUNKS):
        if c < AHEAD:
            send_own(c)
        else:

            @pl.when(edge)
            def _(c=c):
                send_own(c)

    for c in range(CHUNKS):
        for m in range(2):
            arrived(m, z, c)
        for s in range(1, nz):
            for direction in (0, 1):
                b = z - s if direction == 0 else z + s

                @pl.when((b >= 0) & (b < nz))
                def _(b=b, direction=direction):
                    for m in range(2):
                        up(m, b, c).wait_recv()
                        if direction == 0:

                            @pl.when(z < nz - 1)
                            def _():
                                up(m, b, c).start()

                        else:

                            @pl.when(z > 0)
                            def _():
                                down(m, b, c).start()

                        arrived(m, b, c)

        if c + AHEAD < CHUNKS:

            @pl.when(jnp.logical_not(edge))
            def _(c=c):
                send_own(c + AHEAD)

        if c >= 2:
            swap(c - 2)
    for c in range(max(CHUNKS - 2, 0), CHUNKS):
        swap(c)
    for c in range(CHUNKS):
        for m in range(2):
            for b in range(nz):

                @pl.when((z < nz - 1) & (b <= z))
                def _(m=m, b=b):
                    up(m, b, c).wait_send()

                @pl.when((z > 0) & (b >= z))
                def _(m=m, b=b):
                    down(m, b, c).wait_send()

                @pl.when(b != f)
                def _(m=m, b=b):
                    plane(m, b, c).wait_send()

            for g in range(nf):
                pair(m, g, c).wait()


def middle_kernel(
    nf,
    nt,
    factor,
    whole,
    grads,
    gate_weight,
    up_weight,
    down_weight,
    all_out,
    w_out,
    gate_out,
    up_out,
    down_out,
    partial,
    hidden_out,
    landing,
    stage,
    hidden_own,
    sum_send,
    sum_recv,
    up_send,
    down_send,
    line_recv,
    plane_send,
    plane_recv,
    pair_send,
    pair_recv,
    h_send,
    h_recv,
    local_sem,
    w_send,
    w_recv,
):
    f, t = place(nf, nt)
    nz = nt // 2
    z, k = t // 2, lax.rem(t, 2)
    rows = landing.shape[1]
    width = hidden_own.shape[1]

    def block(g):
        return pl.ds(pl.multiple_of(g * rows, rows), rows)

    part = w_out.shape[0]
    ups = (gate_weight, up_weight)

    def into(u, i):
        return w_out.at[:, pl.ds(pl.multiple_of((2 * u + i) * width, width), width)]

    def w_own(i):
        return pltpu.make_async_copy(
            ups[i].at[pl.ds(t * part, part)], into(t, i), local_sem.at[1 + i]
        )

    def multiply(g):
        x = whole[block(g), :]
        partial[block(g), :width] = jnp.dot(x, gate_weight[...], preferred_element_type=F32)
        partial[block(g), width : 2 * width] = jnp.dot(
            x, up_weight[...], preferred_element_type=F32
        )
        partial[block(g), 2 * width :] = lax.dot_general(
            grads[block(g), :],
            down_weight[...],
            (((1,), (1,)), ((), ())),
            preferred_element_type=F32,
        )

    for i in range(2):
        w_own(i).start()
    enter(nf, nt)

    def share(g):
        return remote(
            partial.at[block(g)], landing.at[f], sum_send.at[g], sum_recv.at[f], (g, t)
        )

    def share_in(g):
        return remote(
            partial.at[block(g)], landing.at[g], sum_send.at[g], sum_recv.at[g], (g, t)
        )

    def w_copy(u, i):
        return remote(
            ups[i].at[pl.ds(u * part, part)], into(t, i), w_send.at[u, i], w_recv.at[t, i], (f, u)
        )

    def w_in(u, i):
        return remote(
            ups[i].at[pl.ds(0, part)], into(u, i), w_send.at[u, i], w_recv.at[u, i], (f, u)
        )

    for j in range(1, nt):
        for i in range(2):
            w_copy(lax.rem(t + j, nt), i).start()

    @pl.loop(1, nf + 1)
    def _(j):
        multiply(lax.rem(f + j, nf))

        @pl.when(j > 1)
        def _():
            share(lax.rem(f + j - 1, nf)).start()

    for j in range(1, nf):
        share_in(lax.rem(f + j, nf)).wait_recv()
    total = partial[block(f), :]
    for j in range(1, nf):
        total = total + landing[lax.rem(f + j, nf)]
    gate = total[:, :width]
    up = total[:, width : 2 * width]
    hidden_grad = total[:, 2 * width :]
    squashed = jax.nn.sigmoid(gate)
    activated = gate * squashed
    slope = squashed * (1.0 + gate * (1.0 - squashed))
    stage[0, z, :, :width] = (hidden_grad * up * slope).astype(BF16)
    stage[0, z, :, width:] = (hidden_grad * activated).astype(BF16)
    hidden_own[...] = (activated * up).astype(BF16)

    def h_copy(g):
        return remote(
            hidden_own, hidden_out.at[block(f)], h_send.at[g], h_recv.at[f], (g, t)
        )

    def h_in(g):
        return remote(
            hidden_own, hidden_out.at[block(g)], h_send.at[g], h_recv.at[g], (g, t)
        )

    def spot(g, b):
        at = pl.multiple_of((2 * b + k) * 2 * width, 2 * width)
        return all_out.at[block(g), pl.ds(at, 2 * width)]

    def plane(b, g):
        return remote(
            stage.at[0, b], spot(f, b), plane_send.at[b, g], plane_recv.at[b, f], (g, t)
        )

    def plane_in(b, g):
        return remote(
            stage.at[0, b], spot(g, b), plane_send.at[b, g], plane_recv.at[b, g], (g, t)
        )

    def keep(b):
        return pltpu.make_async_copy(stage.at[0, b], spot(f, b), plane_recv.at[b, f])

    def arrived(m, b):
        for j in range(1, nf):
            plane(b, lax.rem(f + j, nf)).start()
        keep(b).start()

    finish = line_steps(stage, 1, nz, f, t, up_send, down_send, line_recv, arrived)
    for j in range(1, nf):
        h_copy(lax.rem(f + j, nf)).start()
    h_keep = pltpu.make_async_copy(hidden_own, hidden_out.at[block(f)], local_sem.at[0])
    h_keep.start()

    def pair(b, g):
        return remote(
            spot(g, b), spot(g, b), pair_send.at[b, g], pair_recv.at[b, g], (f, t + 1 - 2 * k)
        )

    def pair_in(b, g):
        at = pl.multiple_of((2 * b + 1 - k) * 2 * width, 2 * width)
        here = all_out.at[block(g), pl.ds(at, 2 * width)]
        return remote(
            here, here, pair_send.at[b, g], pair_recv.at[b, g], (f, t + 1 - 2 * k)
        )

    def pass_on(b):
        for j in range(nf):
            g = lax.rem(f + j, nf)
            if j == 0:
                keep(b).wait()
            else:
                plane_in(b, g).wait_recv()
            pair(b, g).start()

    h_keep.wait()
    for j in range(1, nf):
        h_in(lax.rem(f + j, nf)).wait_recv()
    pass_on(z)
    own = pl.ds(pl.multiple_of(t * 2 * width, 2 * width), 2 * width)
    tile = min(TILE, whole.shape[1])
    contract = (((0,), (0,)), ((), ()))

    @pl.loop(0, whole.shape[1] // tile)
    def _(i):
        cols = pl.ds(pl.multiple_of(i * tile, tile), tile)
        term = factor * lax.dot_general(
            whole[:, cols], all_out[:, own], contract, preferred_element_type=F32
        )
        gate_out[cols, :] = term[:, :width]
        up_out[cols, :] = term[:, width:]
        down_out[:, cols] = factor * lax.dot_general(
            hidden_out[...], grads[:, cols], contract, preferred_element_type=F32
        )

    for b in range(nz):

        @pl.when(b != z)
        def _(b=b):
            pass_on(b)

    finish()
    for j in range(1, nf):
        g = lax.rem(f + j, nf)
        share(g).wait_send()
        h_copy(g).wait_send()
        for b in range(nz):
            plane(b, g).wait_send()
    for b in range(nz):
        for g in range(nf):
            pair(b, g).wait_send()
            pair_in(b, g).wait_recv()
    for i in range(2):
        w_own(i).wait()
        for j in range(1, nt):
            u = lax.rem(t + j, nt)
            w_copy(u, i).wait_send()
            w_in(u, i).wait_recv()


def return_kernel(nf, nt, result, out, landing, send, recv, send2, recv2, local_sem):
    f, t = place(nf, nt)
    rows = landing.shape[1]

    def block(g):
        return pl.ds(pl.multiple_of(g * rows, rows), rows)

    keep = pltpu.make_async_copy(result.at[block(f)], landing.at[f], local_sem.at[0])
    keep.start()
    enter(nf, nt)

    def first(g):
        return remote(result.at[block(g)], landing.at[f], send.at[g], recv.at[f], (g, t))

    def first_in(g):
        return remote(result.at[block(g)], landing.at[g], send.at[g], recv.at[g], (g, t))

    for j in range(1, nf):
        first(lax.rem(f + j, nf)).start()
    keep.wait()
    lane = lax.rem(t, nf)

    def second(g):
        return remote(
            landing.at[g], out.at[lane], send2.at[g], recv2.at[lane], (f, 2 * g + t // nf)
        )

    def own(g):
        return pltpu.make_async_copy(landing.at[g], out.at[lane], recv2.at[lane])

    def second_in(i):
        return remote(
            landing.at[0], out.at[i], send2.at[0], recv2.at[i], (f, t)
        )

    for j in range(nf):
        g = lax.rem(f + j, nf)
        if j:
            first_in(g).wait_recv()

        @pl.when(2 * g + t // nf != t)
        def _(g=g):
            second(g).start()

        @pl.when(2 * g + t // nf == t)
        def _(g=g):
            own(g).start()

    source = lax.rem(t, 2) * nf
    for i in range(nf):

        @pl.when(source + i != t)
        def _(i=i):
            second_in(i).wait_recv()

        @pl.when(source + i == t)
        def _(i=i):
            own(0).wait()

    for j in range(nf):
        g = lax.rem(f + j, nf)
        if j:
            first(g).wait_send()

        @pl.when(2 * g + t // nf != t)
        def _(g=g):
            second(g).wait_send()


def params(number):
    return pltpu.CompilerParams(
        collective_id=number, has_side_effects=True, vmem_limit_bytes=VMEM_LIMIT
    )


ANY = pl.BlockSpec(memory_space=pl.ANY)
VMEM = pl.BlockSpec(memory_space=pltpu.VMEM)
DMA = pltpu.SemaphoreType.DMA


def body(tokens, out_grad, gate_weight, up_weight, down_weight):
    nf, nt = lax.axis_size("fsdp"), lax.axis_size("tp")
    nz = nt // 2
    rows, shard = tokens.shape
    depth, width = gate_weight.shape
    count = rows * nf
    factor = 1.0 / math.sqrt(count)
    assert nt == 2 * nf and depth == 2 * shard

    part = depth // nt
    whole, grads = pl.pallas_call(
        functools.partial(spread_kernel, nf, nt),
        out_shape=(
            jax.ShapeDtypeStruct((count, depth), BF16),
            jax.ShapeDtypeStruct((count, depth), BF16),
        ),
        in_specs=[VMEM, VMEM],
        out_specs=(VMEM, VMEM),
        scratch_shapes=[
            pltpu.VMEM((2, nz, rows, shard), BF16),
            DMA((2,)),
            DMA((2, nz, CHUNKS)),
            DMA((2, nz, CHUNKS)),
            DMA((2, nz, CHUNKS)),
            DMA((2, nz, CHUNKS)),
            DMA((2, nf, CHUNKS)),
            DMA((2, nf, CHUNKS)),
            DMA((2, nf, CHUNKS)),
        ],
        compiler_params=params(0),
        name="spread",
    )(tokens, out_grad)

    deltas, turned, gate_grad, up_grad, down_grad = pl.pallas_call(
        functools.partial(middle_kernel, nf, nt, factor),
        out_shape=(
            jax.ShapeDtypeStruct((count, nt * 2 * width), BF16),
            jax.ShapeDtypeStruct((part, nt * 2 * width), BF16),
            jax.ShapeDtypeStruct((depth, width), F32),
            jax.ShapeDtypeStruct((depth, width), F32),
            jax.ShapeDtypeStruct((width, depth), F32),
        ),
        in_specs=[VMEM] * 5,
        out_specs=(VMEM,) * 5,
        scratch_shapes=[
            pltpu.VMEM((count, 3 * width), F32),
            pltpu.VMEM((count, width), BF16),
            pltpu.VMEM((nf, rows, 3 * width), F32),
            pltpu.VMEM((1, nz, rows, 2 * width), BF16),
            pltpu.VMEM((rows, width), BF16),
            DMA((nf,)),
            DMA((nf,)),
            DMA((1, nz)),
            DMA((1, nz)),
            DMA((1, nz)),
            DMA((nz, nf)),
            DMA((nz, nf)),
            DMA((nz, nf)),
            DMA((nz, nf)),
            DMA((nf,)),
            DMA((nf,)),
            DMA((3,)),
            DMA((nt, 2)),
            DMA((nt, 2)),
        ],
        compiler_params=params(1),
        name="middle",
    )(whole, grads, gate_weight, up_weight, down_weight)

    piece = lax.dot_general(
        deltas, turned, (((1,), (1,)), ((), ())), preferred_element_type=F32
    ).astype(BF16)
    input_grad = pl.pallas_call(
        functools.partial(return_kernel, nf, nt),
        out_shape=jax.ShapeDtypeStruct((nf, rows, part), BF16),
        in_specs=[VMEM],
        out_specs=VMEM,
        scratch_shapes=[
            pltpu.VMEM((nf, rows, part), BF16),
            DMA((nf,)),
            DMA((nf,)),
            DMA((nf,)),
            DMA((nf,)),
            DMA((1,)),
        ],
        compiler_params=params(2),
        name="back",
    )(piece)
    input_grad = input_grad.transpose(1, 0, 2).reshape(rows, shard)

    return (input_grad, gate_grad, up_grad, down_grad)


def solution(mesh):
    return jax.shard_map(
        body,
        mesh=mesh,
        in_specs=(
            P("fsdp", "tp"),
            P("fsdp", "tp"),
            P("fsdp", "tp"),
            P("fsdp", "tp"),
            P("tp", "fsdp"),
        ),
        out_specs=(P("fsdp", "tp"), P("fsdp", "tp"), P("fsdp", "tp"), P("tp", "fsdp")),
        check_vma=False,
    )
```

```python
import functools
import math

import jax
import jax.numpy as jnp
from jax import lax
from jax.sharding import PartitionSpec as P
from jax.experimental import pallas as pl
from jax.experimental.pallas import tpu as pltpu

MESH = pl.DeviceIdType.MESH
F32 = jnp.float32
BF16 = jnp.bfloat16
VMEM_LIMIT = 60 * 1024 * 1024
CHUNKS = 4
AHEAD = 2
TILE = 512


def place(nf, nt):
    return lax.axis_index("fsdp"), lax.axis_index("tp")


def enter(nf, nt):
    f, t = place(nf, nt)
    barrier = pltpu.get_barrier_semaphore()
    for j in range(1, nf):
        pl.semaphore_signal(
            barrier, inc=1, device_id=(lax.rem(f + j, nf), t), device_id_type=MESH
        )
    for j in range(1, nt):
        pl.semaphore_signal(
            barrier, inc=1, device_id=(f, lax.rem(t + j, nt)), device_id_type=MESH
        )
    pl.semaphore_wait(barrier, nf + nt - 2)


def remote(src, dst, send, recv, device):
    return pltpu.make_async_remote_copy(
        src_ref=src,
        dst_ref=dst,
        send_sem=send,
        recv_sem=recv,
        device_id=device,
        device_id_type=MESH,
    )


def line_steps(stage, mats, nz, f, t, up_send, down_send, recv, arrived):
    z = t // 2

    def up(m, b):
        return remote(
            stage.at[m, b], stage.at[m, b], up_send.at[m, b], recv.at[m, b], (f, t + 2)
        )

    def down(m, b):
        return remote(
            stage.at[m, b], stage.at[m, b], down_send.at[m, b], recv.at[m, b], (f, t - 2)
        )

    for s in range(nz):
        for m in range(mats):
            for direction in (0, 1) if s else (0,):
                b = z - s if direction == 0 else z + s

                @pl.when((b >= 0) & (b < nz))
                def _(m=m, b=b, s=s, direction=direction):
                    if s:
                        up(m, b).wait_recv()
                    if s == 0 or direction == 0:

                        @pl.when(z < nz - 1)
                        def _():
                            up(m, b).start()

                    if s == 0 or direction == 1:

                        @pl.when(z > 0)
                        def _():
                            down(m, b).start()

                    arrived(m, b)

    def finish():
        for b in range(nz):
            for m in range(mats):

                @pl.when((z < nz - 1) & (b <= z))
                def _(m=m, b=b):
                    up(m, b).wait_send()

                @pl.when((z > 0) & (b >= z))
                def _(m=m, b=b):
                    down(m, b).wait_send()

    return finish


def spread_kernel(
    nf,
    nt,
    tokens,
    grads,
    x_out,
    g_out,
    stage,
    local_sem,
    up_send,
    down_send,
    line_recv,
    plane_send,
    plane_recv,
    pair_send,
    pair_recv,
):
    f, t = place(nf, nt)
    nz = nt // 2
    z, k = t // 2, lax.rem(t, 2)
    rows, width = tokens.shape
    size = rows // CHUNKS
    outs = (x_out, g_out)
    loads = []
    for m, ref in enumerate((tokens, grads)):
        load = pltpu.make_async_copy(ref, stage.at[m, z], local_sem.at[m])
        load.start()
        loads.append(load)
    enter(nf, nt)
    for load in loads:
        load.wait()

    half = pl.ds(pl.multiple_of(k * width, width), width)

    def held(m, b, c):
        return stage.at[m, b, pl.ds(c * size, size)]

    def spot(m, g, c):
        return outs[m].at[pl.ds(pl.multiple_of(g * rows + c * size, size), size), half]

    def up(m, b, c):
        here = held(m, b, c)
        return remote(here, here, up_send.at[m, b, c], line_recv.at[m, b, c], (f, t + 2))

    def down(m, b, c):
        here = held(m, b, c)
        return remote(here, here, down_send.at[m, b, c], line_recv.at[m, b, c], (f, t - 2))

    def plane(m, b, c):
        return remote(
            held(m, b, c), spot(m, f, c), plane_send.at[m, b, c], plane_recv.at[m, f, c], (b, t)
        )

    def plane_in(m, g, c):
        return remote(
            held(m, 0, c), spot(m, g, c), plane_send.at[m, 0, c], plane_recv.at[m, g, c], (f, t)
        )

    def keep(m, c):
        return pltpu.make_async_copy(held(m, f, c), spot(m, f, c), plane_recv.at[m, f, c])

    def arrived(m, b, c):
        @pl.when(b != f)
        def _():
            plane(m, b, c).start()

        @pl.when(b == f)
        def _():
            keep(m, c).start()

    def send_own(c):
        for m in range(2):

            @pl.when(z < nz - 1)
            def _(m=m):
                up(m, z, c).start()

            @pl.when(z > 0)
            def _(m=m):
                down(m, z, c).start()

    def pair(m, g, c):
        here = spot(m, g, c)
        return remote(
            here, here, pair_send.at[m, g, c], pair_recv.at[m, g, c], (f, t + 1 - 2 * k)
        )

    def swap(c):
        for m in range(2):
            for j in range(nf):
                g = lax.rem(f + j, nf)
                if j == 0:
                    keep(m, c).wait()
                else:
                    plane_in(m, g, c).wait_recv()
                pair(m, g, c).start()

    edge = (z == 0) | (z == nz - 1)
    for c in range(CHUNKS):
        if c < AHEAD:
            send_own(c)
        else:

            @pl.when(edge)
            def _(c=c):
                send_own(c)

    for c in range(CHUNKS):
        for m in range(2):
            arrived(m, z, c)
        for s in range(1, nz):
            for direction in (0, 1):
                b = z - s if direction == 0 else z + s

                @pl.when((b >= 0) & (b < nz))
                def _(b=b, direction=direction):
                    for m in range(2):
                        up(m, b, c).wait_recv()
                        if direction == 0:

                            @pl.when(z < nz - 1)
                            def _():
                                up(m, b, c).start()

                        else:

                            @pl.when(z > 0)
                            def _():
                                down(m, b, c).start()

                        arrived(m, b, c)

        if c + AHEAD < CHUNKS:

            @pl.when(jnp.logical_not(edge))
            def _(c=c):
                send_own(c + AHEAD)

        if c >= 2:
            swap(c - 2)
    for c in range(max(CHUNKS - 2, 0), CHUNKS):
        swap(c)
    for c in range(CHUNKS):
        for m in range(2):
            for b in range(nz):

                @pl.when((z < nz - 1) & (b <= z))
                def _(m=m, b=b):
                    up(m, b, c).wait_send()

                @pl.when((z > 0) & (b >= z))
                def _(m=m, b=b):
                    down(m, b, c).wait_send()

                @pl.when(b != f)
                def _(m=m, b=b):
                    plane(m, b, c).wait_send()

            for g in range(nf):
                pair(m, g, c).wait()


def middle_kernel(
    nf,
    nt,
    factor,
    whole,
    grads,
    gate_weight,
    up_weight,
    down_weight,
    all_out,
    w_out,
    gate_out,
    up_out,
    down_out,
    partial,
    hidden_out,
    landing,
    stage,
    hidden_own,
    sum_send,
    sum_recv,
    up_send,
    down_send,
    line_recv,
    plane_send,
    plane_recv,
    pair_send,
    pair_recv,
    h_send,
    h_recv,
    local_sem,
    w_send,
    w_recv,
):
    f, t = place(nf, nt)
    nz = nt // 2
    z, k = t // 2, lax.rem(t, 2)
    rows = landing.shape[1]
    width = hidden_own.shape[1]

    def block(g):
        return pl.ds(pl.multiple_of(g * rows, rows), rows)

    part = w_out.shape[0]
    ups = (gate_weight, up_weight)

    def into(u, i):
        return w_out.at[:, pl.ds(pl.multiple_of((2 * u + i) * width, width), width)]

    def w_own(i):
        return pltpu.make_async_copy(
            ups[i].at[pl.ds(t * part, part)], into(t, i), local_sem.at[1 + i]
        )

    def multiply(g):
        x = whole[block(g), :]
        partial[block(g), :width] = jnp.dot(x, gate_weight[...], preferred_element_type=F32)
        partial[block(g), width : 2 * width] = jnp.dot(
            x, up_weight[...], preferred_element_type=F32
        )
        partial[block(g), 2 * width :] = lax.dot_general(
            grads[block(g), :],
            down_weight[...],
            (((1,), (1,)), ((), ())),
            preferred_element_type=F32,
        )

    for i in range(2):
        w_own(i).start()
    enter(nf, nt)

    def share(g):
        return remote(
            partial.at[block(g)], landing.at[f], sum_send.at[g], sum_recv.at[f], (g, t)
        )

    def share_in(g):
        return remote(
            partial.at[block(g)], landing.at[g], sum_send.at[g], sum_recv.at[g], (g, t)
        )

    def w_copy(u, i):
        return remote(
            ups[i].at[pl.ds(u * part, part)], into(t, i), w_send.at[u, i], w_recv.at[t, i], (f, u)
        )

    def w_in(u, i):
        return remote(
            ups[i].at[pl.ds(0, part)], into(u, i), w_send.at[u, i], w_recv.at[u, i], (f, u)
        )

    for j in range(1, nt):
        for i in range(2):
            w_copy(lax.rem(t + j, nt), i).start()

    @pl.loop(1, nf + 1)
    def _(j):
        multiply(lax.rem(f + j, nf))

        @pl.when(j > 1)
        def _():
            share(lax.rem(f + j - 1, nf)).start()

    for j in range(1, nf):
        share_in(lax.rem(f + j, nf)).wait_recv()
    total = partial[block(f), :]
    for j in range(1, nf):
        total = total + landing[lax.rem(f + j, nf)]
    gate = total[:, :width]
    up = total[:, width : 2 * width]
    hidden_grad = total[:, 2 * width :]
    squashed = jax.nn.sigmoid(gate)
    activated = gate * squashed
    slope = squashed * (1.0 + gate * (1.0 - squashed))
    stage[0, z, :, :width] = (hidden_grad * up * slope).astype(BF16)
    stage[0, z, :, width:] = (hidden_grad * activated).astype(BF16)
    hidden_own[...] = (activated * up).astype(BF16)

    def h_copy(g):
        return remote(
            hidden_own, hidden_out.at[block(f)], h_send.at[g], h_recv.at[f], (g, t)
        )

    def h_in(g):
        return remote(
            hidden_own, hidden_out.at[block(g)], h_send.at[g], h_recv.at[g], (g, t)
        )

    def spot(g, b):
        at = pl.multiple_of((2 * b + k) * 2 * width, 2 * width)
        return all_out.at[block(g), pl.ds(at, 2 * width)]

    def plane(b, g):
        return remote(
            stage.at[0, b], spot(f, b), plane_send.at[b, g], plane_recv.at[b, f], (g, t)
        )

    def plane_in(b, g):
        return remote(
            stage.at[0, b], spot(g, b), plane_send.at[b, g], plane_recv.at[b, g], (g, t)
        )

    def keep(b):
        return pltpu.make_async_copy(stage.at[0, b], spot(f, b), plane_recv.at[b, f])

    def arrived(m, b):
        for j in range(1, nf):
            plane(b, lax.rem(f + j, nf)).start()
        keep(b).start()

    finish = line_steps(stage, 1, nz, f, t, up_send, down_send, line_recv, arrived)
    for j in range(1, nf):
        h_copy(lax.rem(f + j, nf)).start()
    h_keep = pltpu.make_async_copy(hidden_own, hidden_out.at[block(f)], local_sem.at[0])
    h_keep.start()

    def pair(b, g):
        return remote(
            spot(g, b), spot(g, b), pair_send.at[b, g], pair_recv.at[b, g], (f, t + 1 - 2 * k)
        )

    def pair_in(b, g):
        at = pl.multiple_of((2 * b + 1 - k) * 2 * width, 2 * width)
        here = all_out.at[block(g), pl.ds(at, 2 * width)]
        return remote(
            here, here, pair_send.at[b, g], pair_recv.at[b, g], (f, t + 1 - 2 * k)
        )

    def pass_on(b):
        for j in range(nf):
            g = lax.rem(f + j, nf)
            if j == 0:
                keep(b).wait()
            else:
                plane_in(b, g).wait_recv()
            pair(b, g).start()

    h_keep.wait()
    for j in range(1, nf):
        h_in(lax.rem(f + j, nf)).wait_recv()
    pass_on(z)
    own = pl.ds(pl.multiple_of(t * 2 * width, 2 * width), 2 * width)
    tile = min(TILE, whole.shape[1])
    contract = (((0,), (0,)), ((), ()))

    @pl.loop(0, whole.shape[1] // tile)
    def _(i):
        cols = pl.ds(pl.multiple_of(i * tile, tile), tile)
        term = factor * lax.dot_general(
            whole[:, cols], all_out[:, own], contract, preferred_element_type=F32
        )
        gate_out[cols, :] = term[:, :width]
        up_out[cols, :] = term[:, width:]
        down_out[:, cols] = factor * lax.dot_general(
            hidden_out[...], grads[:, cols], contract, preferred_element_type=F32
        )

    for b in range(nz):

        @pl.when(b != z)
        def _(b=b):
            pass_on(b)

    finish()
    for j in range(1, nf):
        g = lax.rem(f + j, nf)
        share(g).wait_send()
        h_copy(g).wait_send()
        for b in range(nz):
            plane(b, g).wait_send()
    for b in range(nz):
        for g in range(nf):
            pair(b, g).wait_send()
            pair_in(b, g).wait_recv()
    for i in range(2):
        w_own(i).wait()
        for j in range(1, nt):
            u = lax.rem(t + j, nt)
            w_copy(u, i).wait_send()
            w_in(u, i).wait_recv()


def return_kernel(nf, nt, deltas, turned, out, result, landing, send, recv, send2, recv2, local_sem):
    f, t = place(nf, nt)
    rows = landing.shape[1]

    def block(g):
        return pl.ds(pl.multiple_of(g * rows, rows), rows)

    keep = pltpu.make_async_copy(result.at[block(f)], landing.at[f], local_sem.at[0])
    enter(nf, nt)

    def first(g):
        return remote(result.at[block(g)], landing.at[f], send.at[g], recv.at[f], (g, t))

    def first_in(g):
        return remote(result.at[block(g)], landing.at[g], send.at[g], recv.at[g], (g, t))

    @pl.loop(1, nf + 1)
    def _(j):
        g = lax.rem(f + j, nf)
        result[block(g), :] = lax.dot_general(
            deltas[block(g), :],
            turned[...],
            (((1,), (1,)), ((), ())),
            preferred_element_type=F32,
        ).astype(BF16)

        @pl.when(j > 1)
        def _():
            first(lax.rem(f + j - 1, nf)).start()

    keep.start()
    keep.wait()
    lane = lax.rem(t, nf)

    def second(g):
        return remote(
            landing.at[g], out.at[lane], send2.at[g], recv2.at[lane], (f, 2 * g + t // nf)
        )

    def own(g):
        return pltpu.make_async_copy(landing.at[g], out.at[lane], recv2.at[lane])

    def second_in(i):
        return remote(
            landing.at[0], out.at[i], send2.at[0], recv2.at[i], (f, t)
        )

    for j in range(nf):
        g = lax.rem(f + j, nf)
        if j:
            first_in(g).wait_recv()

        @pl.when(2 * g + t // nf != t)
        def _(g=g):
            second(g).start()

        @pl.when(2 * g + t // nf == t)
        def _(g=g):
            own(g).start()

    source = lax.rem(t, 2) * nf
    for i in range(nf):

        @pl.when(source + i != t)
        def _(i=i):
            second_in(i).wait_recv()

        @pl.when(source + i == t)
        def _(i=i):
            own(0).wait()

    for j in range(nf):
        g = lax.rem(f + j, nf)
        if j:
            first(g).wait_send()

        @pl.when(2 * g + t // nf != t)
        def _(g=g):
            second(g).wait_send()


def params(number):
    return pltpu.CompilerParams(
        collective_id=number, has_side_effects=True, vmem_limit_bytes=VMEM_LIMIT
    )


ANY = pl.BlockSpec(memory_space=pl.ANY)
VMEM = pl.BlockSpec(memory_space=pltpu.VMEM)
DMA = pltpu.SemaphoreType.DMA


def body(tokens, out_grad, gate_weight, up_weight, down_weight):
    nf, nt = lax.axis_size("fsdp"), lax.axis_size("tp")
    nz = nt // 2
    rows, shard = tokens.shape
    depth, width = gate_weight.shape
    count = rows * nf
    factor = 1.0 / math.sqrt(count)
    assert nt == 2 * nf and depth == 2 * shard

    part = depth // nt
    whole, grads = pl.pallas_call(
        functools.partial(spread_kernel, nf, nt),
        out_shape=(
            jax.ShapeDtypeStruct((count, depth), BF16),
            jax.ShapeDtypeStruct((count, depth), BF16),
        ),
        in_specs=[VMEM, VMEM],
        out_specs=(VMEM, VMEM),
        scratch_shapes=[
            pltpu.VMEM((2, nz, rows, shard), BF16),
            DMA((2,)),
            DMA((2, nz, CHUNKS)),
            DMA((2, nz, CHUNKS)),
            DMA((2, nz, CHUNKS)),
            DMA((2, nz, CHUNKS)),
            DMA((2, nf, CHUNKS)),
            DMA((2, nf, CHUNKS)),
            DMA((2, nf, CHUNKS)),
        ],
        compiler_params=params(0),
        name="spread",
    )(tokens, out_grad)

    deltas, turned, gate_grad, up_grad, down_grad = pl.pallas_call(
        functools.partial(middle_kernel, nf, nt, factor),
        out_shape=(
            jax.ShapeDtypeStruct((count, nt * 2 * width), BF16),
            jax.ShapeDtypeStruct((part, nt * 2 * width), BF16),
            jax.ShapeDtypeStruct((depth, width), F32),
            jax.ShapeDtypeStruct((depth, width), F32),
            jax.ShapeDtypeStruct((width, depth), F32),
        ),
        in_specs=[VMEM] * 5,
        out_specs=(VMEM,) * 5,
        scratch_shapes=[
            pltpu.VMEM((count, 3 * width), F32),
            pltpu.VMEM((count, width), BF16),
            pltpu.VMEM((nf, rows, 3 * width), F32),
            pltpu.VMEM((1, nz, rows, 2 * width), BF16),
            pltpu.VMEM((rows, width), BF16),
            DMA((nf,)),
            DMA((nf,)),
            DMA((1, nz)),
            DMA((1, nz)),
            DMA((1, nz)),
            DMA((nz, nf)),
            DMA((nz, nf)),
            DMA((nz, nf)),
            DMA((nz, nf)),
            DMA((nf,)),
            DMA((nf,)),
            DMA((3,)),
            DMA((nt, 2)),
            DMA((nt, 2)),
        ],
        compiler_params=params(1),
        name="middle",
    )(whole, grads, gate_weight, up_weight, down_weight)

    input_grad = pl.pallas_call(
        functools.partial(return_kernel, nf, nt),
        out_shape=jax.ShapeDtypeStruct((nf, rows, part), BF16),
        in_specs=[VMEM, VMEM],
        out_specs=VMEM,
        scratch_shapes=[
            pltpu.VMEM((count, part), BF16),
            pltpu.VMEM((nf, rows, part), BF16),
            DMA((nf,)),
            DMA((nf,)),
            DMA((nf,)),
            DMA((nf,)),
            DMA((1,)),
        ],
        compiler_params=params(2),
        name="back",
    )(deltas, turned)
    input_grad = input_grad.transpose(1, 0, 2).reshape(rows, shard)

    return (input_grad, gate_grad, up_grad, down_grad)


def solution(mesh):
    return jax.shard_map(
        body,
        mesh=mesh,
        in_specs=(
            P("fsdp", "tp"),
            P("fsdp", "tp"),
            P("fsdp", "tp"),
            P("fsdp", "tp"),
            P("tp", "fsdp"),
        ),
        out_specs=(P("fsdp", "tp"), P("fsdp", "tp"), P("fsdp", "tp"), P("tp", "fsdp")),
        check_vma=False,
    )
```
